512 devices in a mesh: gx: 8 (over y, core), gy: 16 (over z), gz: 4 (over x).
Axes of the slice: x: 4, y: 4, z: 16, core: 2. Of those that a mesh axis runs over, the one named last changes fastest.
Arguments:
- a_vals: float32 [16, 16, 4, 6, 128, 128], P('gy', 'gx', 'gz'), may hold values from -0.25 to 0.25
- a_cols: int32 [16, 16, 4, 6], P('gy', 'gx', 'gz'), may hold values from 0 to 63, as said below
- a_count: int32 [16, 16, 4], P('gy', 'gx', 'gz'), may hold values from 1 to 6, as said below
- p_vals: float32 [4, 64, 8, 1, 128, 128], P('gz', 'gy', 'gx'), may hold values from -6 to 6
- p_cols: int32 [4, 64, 8, 1], P('gz', 'gy', 'gx'), may hold values from 0 to 1, as said below
- p_count: int32 [4, 64, 8], P('gz', 'gy', 'gx'), may hold values from 0 to 1, as said below
Outputs:
- c_tiles: float32 [32768, 2048], P(('gy', 'gz'), 'gx')
The draws below stay inside these ranges and needn't reach their ends.
Inputs may be any that keep to these rules, and one draw needn't show every extreme that they name: `a_cols`: inner tile indices of one block row and slice are distinct across its 6 slots. Slots 0 to a_count - 1 are live; the block rows of every device include one with all 6 slots live. `p_cols`: column tiles of one block row and group are distinct across its 1 slots. Slots 0 to p_count - 1 are live; the block rows of every device include one with all 1 slots live.
All inputs are finite; a program needn't handle non-finite values.
Results may differ from the reference program's by a relative error of at most 0.0003.
Values sent between devices are 32-bit elements; how exact they have to be, the bound alone decides.
No kernel may reach another device: no remote copies, remote signals or barrier semaphores. Data moves between devices by JAX's collectives and lax.ppermute only.
A program may use at most 128 MiB of HBM per device.

```python
import jax
import jax.numpy as jnp
from jax import lax

TILE = 128
ROWS_DEV = 2
SLOTS_A = 6
SLOTS_P = 1
COLS_DEV = 2
RX = 16
KZ = 64
N_GX = 8
N_GY = 16
N_GZ = 4


def draw_a_count(key, part):
    first = jax.random.randint(jax.random.fold_in(key, 11), (N_GY, RX, N_GZ), 1, SLOTS_A + 1)
    second = jax.random.randint(jax.random.fold_in(key, 12), (N_GY, RX, N_GZ), 1, SLOTS_A + 1)
    counts = jnp.minimum(first, second)
    picked = jax.random.randint(jax.random.fold_in(key, 13), (N_GY, RX // ROWS_DEV, 1, N_GZ), 0, ROWS_DEV)
    position = jnp.arange(ROWS_DEV, dtype=jnp.int32)[None, None, :, None]
    filled = (position == picked).reshape(N_GY, RX, N_GZ)
    return jnp.where(filled, SLOTS_A, counts).astype(jnp.int32)


def draw_a_cols(key, part):
    line_total = N_GY * RX * N_GZ
    base = jnp.broadcast_to(jnp.arange(KZ, dtype=jnp.int32), (line_total, KZ))
    mixed = jax.random.permutation(jax.random.fold_in(key, 21), base, axis=1, independent=True)
    return mixed[:, :SLOTS_A].reshape(N_GY, RX, N_GZ, SLOTS_A).astype(jnp.int32)


def draw_p_count(key, part):
    counts = jax.random.randint(jax.random.fold_in(key, 31), (N_GZ, KZ, N_GX), 0, SLOTS_P + 1)
    block_rows = KZ // N_GY
    picked = jax.random.randint(jax.random.fold_in(key, 32), (N_GZ, N_GY, 1, N_GX), 0, block_rows)
    position = jnp.arange(block_rows, dtype=jnp.int32)[None, None, :, None]
    filled = (position == picked).reshape(N_GZ, KZ, N_GX)
    return jnp.where(filled, SLOTS_P, counts).astype(jnp.int32)


def draw_p_cols(key, part):
    line_total = N_GZ * KZ * N_GX
    base = jnp.broadcast_to(jnp.arange(COLS_DEV, dtype=jnp.int32), (line_total, COLS_DEV))
    mixed = jax.random.permutation(jax.random.fold_in(key, 41), base, axis=1, independent=True)
    return mixed[:, :SLOTS_P].reshape(N_GZ, KZ, N_GX, SLOTS_P).astype(jnp.int32)


def shard_levels(rng, dims, cuts, least, largest):
    loudness = 1.0
    for dim, blocks in cuts:
        steps = jax.random.uniform(jax.random.fold_in(jax.random.fold_in(rng, 6), dim), (blocks,), jnp.float32, least / len(cuts), largest / len(cuts))
        loudness = loudness * jnp.repeat(jnp.exp(steps), dims[dim] // blocks).reshape((-1,) + (1,) * (len(dims) - 1 - dim))
    return loudness


def noise(own_key, shape, width, bound, cuts=(), kind=jnp.bfloat16):
    values = width * jax.random.normal(own_key, shape, jnp.float32)
    if cuts:
        values = values * shard_levels(own_key, shape, cuts, -0.22, 0.18)
    return jnp.clip(values, -bound, bound).astype(kind)


def setup_inputs(seed: int = 0) -> dict:
    key_of = jax.random.split(jax.random.key(seed), 7)
    a_vals = noise(key_of[0], (N_GY, RX, N_GZ, SLOTS_A, TILE, TILE), (4 * TILE) ** -0.5, 0.25, ((0, 16), (1, 8), (2, 4)), jnp.float32)
    a_cols = draw_a_cols(jax.random.fold_in(key_of[6], 71), 0)
    a_count = draw_a_count(jax.random.fold_in(key_of[6], 71), 0)
    p_vals = noise(key_of[3], (N_GZ, KZ, N_GX, SLOTS_P, TILE, TILE), 1.0, 6.0, ((0, 4), (1, 16), (2, 8)), jnp.float32)
    p_cols = draw_p_cols(jax.random.fold_in(key_of[6], 71), 0)
    p_count = draw_p_count(jax.random.fold_in(key_of[6], 71), 0)
    return dict(a_vals=a_vals, a_cols=a_cols, a_count=a_count, p_vals=p_vals, p_cols=p_cols, p_count=p_count)


def reference(a_vals, a_cols, a_count, p_vals, p_cols, p_count):
    tile_size = a_vals.shape[-1]
    groups_y, rows_x, slices, slots_a = a_cols.shape
    inner_rows = p_cols.shape[1]
    groups_x = p_cols.shape[2]
    slots_p = p_cols.shape[3]
    rows_all = groups_y * rows_x
    a_values = a_vals.reshape(rows_all, slices, slots_a, tile_size, tile_size)
    a_columns = a_cols.reshape(rows_all, slices, slots_a)
    a_counts = a_count.reshape(rows_all, slices)
    p_values = p_vals.reshape(slices * inner_rows, groups_x, slots_p, tile_size, tile_size)
    alive_p = jnp.arange(slots_p, dtype=jnp.int32) < p_count[..., None]
    matches = p_cols[..., None] == jnp.arange(COLS_DEV, dtype=jnp.int32)
    p_weights = (alive_p[..., None] & matches).astype(jnp.float32)
    p_weights = p_weights.reshape(slices * inner_rows, groups_x, slots_p, COLS_DEV)
    offsets = (jnp.arange(slices, dtype=jnp.int32) * inner_rows)[:, None]

    def one_row(row_index):
        alive_a = jnp.arange(slots_a, dtype=jnp.int32) < a_counts[row_index][:, None]
        tile_part = jnp.where(alive_a[..., None, None], a_values[row_index], 0.0)
        indices = a_columns[row_index].astype(jnp.int32) + offsets
        chosen = p_values[indices]
        weights = p_weights[indices]
        product = jnp.einsum("zsij,zsxpjk->zsxpik", tile_part, chosen, precision=lax.Precision.HIGHEST)
        placed = jnp.einsum("zsxpc,zsxpik->ixck", weights, product, precision=lax.Precision.HIGHEST)
        return placed.reshape(tile_size, groups_x * COLS_DEV * tile_size)

    result = lax.map(one_row, jnp.arange(rows_all, dtype=jnp.int32))
    return result.reshape(rows_all * tile_size, groups_x * COLS_DEV * tile_size)
```

```python
import functools

import jax
import jax.numpy as jnp
from jax import lax
from jax.experimental import pallas as pl
from jax.experimental.pallas import tpu as pltpu
from jax.sharding import PartitionSpec as P


TILE = 128
SLOTS = 6
NY = 4
NZ = 16
NX = 4
PB = 4
BF = jnp.bfloat16
F32 = jnp.float32


def along_z(v, step):
    return lax.ppermute(v, "gy", [(i, (i + step) % NZ) for i in range(NZ)])


def along_y(v, step):
    n = 2 * NY
    return lax.ppermute(v, "gx", [(i, (i + 2 * step) % n) for i in range(n)])


def partner(v):
    return lax.ppermute(v, "gx", [(i, i ^ 1) for i in range(2 * NY)])


def after(v, other):
    return lax.optimization_barrier((v, other))[0]


def along_x(v, step):
    pairs = []
    for x in range(2 * NY):
        for z in range(NX):
            to = z + step if x % 2 == 0 else z - step
            pairs.append((x * NX + z, x * NX + to % NX))
    return lax.ppermute(v, ("gx", "gz"), pairs)


def with_row(values, codes):
    row = lax.pad(codes.reshape(1, -1), jnp.float32(0), ((0, 7, 0), (0, TILE - codes.size, 0)))
    return jnp.concatenate([values, row], axis=0)


def split(t):
    hi = t.astype(BF)
    return hi, (t - hi.astype(F32)).astype(BF)


def prep_p_kernel(*refs):
    blocks, (hi_ref, lo_ref) = refs[:NZ], refs[NZ:]
    me = lax.axis_index("gy")
    for b in range(NZ):
        off = -b if b <= 8 else b - 8
        src = lax.rem(me + off + NZ, NZ)
        for j in range(PB):
            t = blocks[b][j * TILE : (j + 1) * TILE, :]
            code = blocks[b][PB * TILE : PB * TILE + 1, j : j + 1]
            hi, lo = split(t)
            k = src * PB + j
            for c in range(2):
                keep = code == float(c + 1)
                hi_ref[k, :, c * TILE : (c + 1) * TILE] = jnp.where(keep, hi, jnp.zeros_like(hi))
                lo_ref[k, :, c * TILE : (c + 1) * TILE] = jnp.where(keep, lo, jnp.zeros_like(lo))


A_ROWS = 2 * SLOTS * TILE + 8


def products_kernel(d, code_ref, mine_ref, theirs_ref, ph_ref, pl_ref, out_ref, tiles, sems):
    gx = lax.axis_index("gx")
    odd = lax.rem(gx, 2)
    owner = lax.rem(lax.axis_index("gz") + (1 - 2 * odd) * d + NX, NX)
    rel = lax.rem(owner - gx // 2 + NY, NY)
    b = jnp.where(rel == 0, 0, jnp.where(rel == 1, 2, jnp.where(rel == 2, 3, 1)))
    row = pl.multiple_of(b * A_ROWS, 8)
    copies = [
        pltpu.make_async_copy(ref.at[pl.ds(row, A_ROWS - 8)], tiles.at[c], sems.at[c])
        for c, ref in enumerate((mine_ref, theirs_ref))
    ]
    for copy in copies:
        copy.start()
    for c in range(2):
        copies[c].wait()
        core = odd if c == 0 else 1 - odd

        def one(i, _, c=c, core=core):
            top = jnp.zeros((2 * TILE, 2 * TILE), F32)
            low = jnp.zeros((TILE, 2 * TILE), F32)
            for q in range(SLOTS // 2):
                his, los, rhs, rls = [], [], [], []
                for s in (2 * q, 2 * q + 1):
                    code = code_ref[(c * NY + b) * 2 + i, s]
                    t = tiles[c, pl.ds(pl.multiple_of((i * SLOTS + s) * TILE, TILE), TILE), :]
                    hi, lo = split(jnp.where(code >= 0, t, 0.0))
                    k = jnp.maximum(code, 0)
                    his.append(hi)
                    los.append(lo)
                    rhs.append(ph_ref[k])
                    rls.append(pl_ref[k])
                ah = jnp.concatenate(his, axis=1)
                both = jnp.concatenate([ah, jnp.concatenate(los, axis=1)], axis=0)
                top = top + jnp.dot(both, jnp.concatenate(rhs, axis=0), preferred_element_type=F32)
                low = low + jnp.dot(ah, jnp.concatenate(rls, axis=0), preferred_element_type=F32)
            r = pl.multiple_of((core * 2 + i) * TILE, TILE)
            out_ref[pl.ds(r, TILE), :] = top[:TILE] + top[TILE:] + low
            return 0

        lax.fori_loop(0, 2, one, 0)


def body(a_vals, a_cols, a_count, p_vals, p_cols, p_count):
    rows = a_vals.shape[1]
    alive = jnp.arange(SLOTS, dtype=jnp.int32) < a_count[0, :, 0][:, None]
    a_codes = jnp.where(alive, a_cols[0, :, 0], -1).astype(F32)
    p_codes = jnp.where(p_count[0, :, 0] > 0, p_cols[0, :, 0, 0] + 1, 0).astype(F32)
    own_p = with_row(p_vals.reshape(PB * TILE, TILE), p_codes)
    a_row = lax.pad(a_codes, jnp.float32(0), ((0, 8 - rows, 0), (0, TILE - SLOTS, 0)))
    low, high = [own_p], [own_p]
    for t in range(8):
        low.append(along_z(after(low[t], high[t - 1]) if t > 1 else low[t], 1))
        if t < 7:
            high.append(along_z(after(high[t], low[t]) if t > 0 else high[t], -1))

    a_flat = after(a_vals, low[1]).reshape(rows * SLOTS * TILE, TILE)
    own_a = jnp.concatenate([a_flat, a_row], axis=0)
    up = along_y(own_a, 1)
    down = along_y(after(own_a, low[2]), -1)
    far = along_y(after(up, low[4]), 1)
    mine = jnp.concatenate([own_a, up, down, far], axis=0)
    theirs = partner(after(mine, low[6]))
    codes = jnp.stack([mine, theirs]).reshape(2, NY, A_ROWS, TILE)
    codes = codes[:, :, A_ROWS - 8 : A_ROWS - 6, :SLOTS].astype(jnp.int32).reshape(4 * NX, SLOTS)

    vm = pl.BlockSpec(memory_space=pltpu.VMEM)
    sm = pl.BlockSpec(memory_space=pltpu.SMEM)
    params = pltpu.CompilerParams(vmem_limit_bytes=8 * 2**20)
    ph, plo = pl.pallas_call(
        prep_p_kernel,
        out_shape=[jax.ShapeDtypeStruct((NZ * PB, TILE, 2 * TILE), BF)] * 2,
        in_specs=[vm] * NZ,
        out_specs=[vm] * 2,
        compiler_params=params,
        name="prep_p",
    )(*(low + high[1:]))

    hbm = pl.BlockSpec(memory_space=pltpu.HBM)

    def share(d, codes):
        return pl.pallas_call(
            functools.partial(products_kernel, d),
            out_shape=jax.ShapeDtypeStruct((4 * TILE, 2 * TILE), F32),
            in_specs=[sm, hbm, hbm, vm, vm],
            out_specs=vm,
            scratch_shapes=[
                pltpu.VMEM((2, A_ROWS - 8, TILE), F32),
                pltpu.SemaphoreType.DMA((2,)),
            ],
            compiler_params=params,
            cost_estimate=pl.CostEstimate(
                flops=12 * 10**9, bytes_accessed=4 * 2**20, transcendentals=0
            ),
            name="products",
        )(codes, mine, theirs, ph, plo)

    c2 = share(2, codes)
    r1 = along_x(c2, 1)
    c3 = share(-1, after(codes, c2))
    r2 = along_x(c3, -1)
    c1 = share(1, after(codes, c3))
    r3 = along_x(c1 + r1, 1)
    c0 = share(0, after(codes, c1))
    return c0 + r2 + r3


def solution(mesh):
    placed = (
        P("gy", "gx", "gz", None, None, None),
        P("gy", "gx", "gz", None),
        P("gy", "gx", "gz"),
        P("gz", "gy", "gx", None, None, None),
        P("gz", "gy", "gx", None),
        P("gz", "gy", "gx"),
    )
    return jax.shard_map(
        body, mesh=mesh, in_specs=placed, out_specs=P(("gy", "gz"), "gx"), check_vma=False
    )
```

```python
import functools

import jax
import jax.numpy as jnp
from jax import lax
from jax.experimental import pallas as pl
from jax.experimental.pallas import tpu as pltpu
from jax.sharding import PartitionSpec as P


TILE = 128
SLOTS = 6
NY = 4
NZ = 16
NX = 4
PB = 4
BF = jnp.bfloat16
F32 = jnp.float32


def along_y(v, step):
    n = 2 * NY
    return lax.ppermute(v, "gx", [(i, (i + 2 * step) % n) for i in range(n)])


def partner(v):
    return lax.ppermute(v, "gx", [(i, i ^ 1) for i in range(2 * NY)])


def after(v, other):
    return lax.optimization_barrier((v, other))[0]


def along_x(v, step):
    pairs = []
    for x in range(2 * NY):
        for z in range(NX):
            to = z + step if x % 2 == 0 else z - step
            pairs.append((x * NX + z, x * NX + to % NX))
    return lax.ppermute(v, ("gx", "gz"), pairs)


def with_row(values, codes):
    row = lax.pad(codes.reshape(1, -1), jnp.float32(0), ((0, 7, 0), (0, TILE - codes.size, 0)))
    return jnp.concatenate([values, row], axis=0)


def split(t):
    hi = t.astype(BF)
    return hi, (t - hi.astype(F32)).astype(BF)


P_ROWS = PB * TILE + 8
DEPTH = 4


def prep_p_kernel(all_ref, hi_ref, lo_ref, blocks, sems):
    copies = [
        pltpu.make_async_copy(all_ref.at[pl.ds(b * P_ROWS, P_ROWS)], blocks.at[b], sems.at[b])
        for b in range(NZ)
    ]
    for copy in copies[:DEPTH]:
        copy.start()
    for b in range(NZ):
        copies[b].wait()
        if b + DEPTH < NZ:
            copies[b + DEPTH].start()
        for j in range(PB):
            t = blocks[b, j * TILE : (j + 1) * TILE, :]
            code = blocks[b, PB * TILE : PB * TILE + 1, j : j + 1]
            hi, lo = split(t)
            for c in range(2):
                keep = code == float(c + 1)
                part = slice(c * TILE, (c + 1) * TILE)
                hi_ref[b * PB + j, :, part] = jnp.where(keep, hi, jnp.zeros_like(hi))
                lo_ref[b * PB + j, :, part] = jnp.where(keep, lo, jnp.zeros_like(lo))


A_ROWS = 2 * SLOTS * TILE + 8


def products_kernel(d, code_ref, mine_ref, theirs_ref, ph_ref, pl_ref, out_ref):
    gx = lax.axis_index("gx")
    odd = lax.rem(gx, 2)
    owner = lax.rem(lax.axis_index("gz") + (1 - 2 * odd) * d + NX, NX)
    rel = lax.rem(owner - gx // 2 + NY, NY)
    b = jnp.where(rel == 0, 0, jnp.where(rel == 1, 2, jnp.where(rel == 2, 3, 1)))
    for c, ref in enumerate((mine_ref, theirs_ref)):
        core = odd if c == 0 else 1 - odd

        def one(i, _, c=c, core=core, ref=ref):
            top = jnp.zeros((2 * TILE, 2 * TILE), F32)
            low = jnp.zeros((TILE, 2 * TILE), F32)
            for q in range(SLOTS // 2):
                his, los, rhs, rls = [], [], [], []
                for s in (2 * q, 2 * q + 1):
                    code = code_ref[(c * NY + b) * 2 + i, s]
                    t = ref[pl.ds(pl.multiple_of(b * A_ROWS + (i * SLOTS + s) * TILE, 8), TILE), :]
                    hi, lo = split(jnp.where(code >= 0, t, 0.0))
                    k = jnp.maximum(code, 0)
                    his.append(hi)
                    los.append(lo)
                    rhs.append(ph_ref[k])
                    rls.append(pl_ref[k])
                ah = jnp.concatenate(his, axis=1)
                both = jnp.concatenate([ah, jnp.concatenate(los, axis=1)], axis=0)
                top = top + jnp.dot(both, jnp.concatenate(rhs, axis=0), preferred_element_type=F32)
                low = low + jnp.dot(ah, jnp.concatenate(rls, axis=0), preferred_element_type=F32)
            r = pl.multiple_of((core * 2 + i) * TILE, TILE)
            out_ref[pl.ds(r, TILE), :] = top[:TILE] + top[TILE:] + low
            return 0

        lax.fori_loop(0, 2, one, 0)


def body(a_vals, a_cols, a_count, p_vals, p_cols, p_count):
    rows = a_vals.shape[1]
    alive = jnp.arange(SLOTS, dtype=jnp.int32) < a_count[0, :, 0][:, None]
    a_codes = jnp.where(alive, a_cols[0, :, 0], -1).astype(F32)
    p_codes = jnp.where(p_count[0, :, 0] > 0, p_cols[0, :, 0, 0] + 1, 0).astype(F32)
    own_p = with_row(p_vals.reshape(PB * TILE, TILE), p_codes)
    a_row = lax.pad(a_codes, jnp.float32(0), ((0, 8 - rows, 0), (0, TILE - SLOTS, 0)))
    p_all = lax.all_gather(own_p, "gy", axis=0, tiled=True)
    a_flat = after(a_vals, own_p).reshape(rows * SLOTS * TILE, TILE)
    own_a = jnp.concatenate([a_flat, a_row], axis=0)
    up = along_y(own_a, 1)
    down = along_y(own_a, -1)
    far = along_y(up, 1)
    mine = jnp.concatenate([own_a, up, down, far], axis=0)
    theirs = partner(mine)
    codes = jnp.stack([mine, theirs]).reshape(2, NY, A_ROWS, TILE)
    codes = codes[:, :, A_ROWS - 8 : A_ROWS - 6, :SLOTS].astype(jnp.int32).reshape(4 * NX, SLOTS)

    vm = pl.BlockSpec(memory_space=pltpu.VMEM)
    sm = pl.BlockSpec(memory_space=pltpu.SMEM)
    params = pltpu.CompilerParams(vmem_limit_bytes=10 * 2**20)
    hbm = pl.BlockSpec(memory_space=pltpu.HBM)
    ph, plo = pl.pallas_call(
        prep_p_kernel,
        out_shape=[jax.ShapeDtypeStruct((NZ * PB, TILE, 2 * TILE), BF)] * 2,
        in_specs=[hbm],
        out_specs=[vm] * 2,
        scratch_shapes=[pltpu.VMEM((NZ, P_ROWS, TILE), F32), pltpu.SemaphoreType.DMA((NZ,))],
        compiler_params=pltpu.CompilerParams(vmem_limit_bytes=44 * 2**20),
        name="prep_p",
    )(p_all)

    def share(d, codes):
        return pl.pallas_call(
            functools.partial(products_kernel, d),
            out_shape=jax.ShapeDtypeStruct((4 * TILE, 2 * TILE), F32),
            in_specs=[sm, vm, vm, vm, vm],
            out_specs=vm,
            compiler_params=params,
            cost_estimate=pl.CostEstimate(
                flops=12 * 10**9, bytes_accessed=4 * 2**20, transcendentals=0
            ),
            name="products",
        )(codes, mine, theirs, ph, plo)

    c2 = share(2, codes)
    r1 = along_x(c2, 1)
    c3 = share(-1, after(codes, c2))
    r2 = along_x(c3, -1)
    c1 = share(1, after(codes, c3))
    r3 = along_x(c1 + r1, 1)
    c0 = share(0, after(codes, c1))
    return c0 + r2 + r3


def solution(mesh):
    placed = (
        P("gy", "gx", "gz", None, None, None),
        P("gy", "gx", "gz", None),
        P("gy", "gx", "gz"),
        P("gz", "gy", "gx", None, None, None),
        P("gz", "gy", "gx", None),
        P("gz", "gy", "gx"),
    )
    return jax.shard_map(
        body, mesh=mesh, in_specs=placed, out_specs=P(("gy", "gz"), "gx"), check_vma=False
    )
```
